32 devices in a mesh: seq: 2 (over x), head: 4 (over z), dp: 4 (over y, core).
Axes of the slice: x: 2, y: 2, z: 4, core: 2. Of those that a mesh axis runs over, the one named last changes fastest.
Arguments:
- queries: bfloat16 [4, 512, 64, 128], P('dp', 'seq', 'head'), may hold values from -6 to 6
- keys: bfloat16 [4, 512, 8, 128], P('dp', 'seq', 'head'), may hold values from -6 to 6
- values: bfloat16 [4, 512, 8, 128], P('dp', 'seq', 'head'), may hold values from -6 to 6
- attn_out: bfloat16 [4, 512, 64, 128], P('dp', 'seq', 'head'), may hold values from -6 to 6
- out_grad: bfloat16 [4, 512, 64, 128], P('dp', 'seq', 'head'), may hold values from -6 to 6
- gate_values: float32 [4, 64, 512], P('dp', 'head', 'seq'), may hold values from 0.05 to 0.95
- log_totals: float32 [4, 64, 512], P('dp', 'head', 'seq'), may hold values from 3 to 5
- hidden: bfloat16 [4, 512, 5120], P('dp', 'seq', 'head'), may hold values from -6 to 6
- block_ids: int32 [4, 8, 8, 16], P('dp', 'seq', 'head'), may hold values from 0 to 7, as said below
- block_valid: int32 [4, 8, 8, 16], P('dp', 'seq', 'head'), may hold values from 0 to 1
Outputs:
- query_grad: bfloat16 [4, 512, 64, 128], P('dp', 'seq', 'head')
- key_grad: bfloat16 [4, 512, 8, 128], P('dp', 'seq', 'head')
- value_grad: bfloat16 [4, 512, 8, 128], P('dp', 'seq', 'head')
- gate_weight_grad: float32 [64, 5120], P(None, 'head')
The draws below stay inside these ranges and needn't reach their ends.
Inputs may be any that keep to these rules, and one draw needn't show every extreme that they name: `block_ids`: for query tile t and key head k, the slots whose block_valid is 1 name distinct blocks of index at most t, among them block t itself and block 0; exactly min(16, t + 1) slots are valid. The ids of the other slots are any blocks, and may repeat a valid one.
All inputs are finite; a program needn't handle non-finite values.
Results may differ from the reference program's by a relative error of at most 0.025.
Values may be sent and summed in bfloat16 or wider, within the bound.
A program may use at most 128 MiB of HBM per device.

```python
import jax
import jax.numpy as jnp
from jax import lax

D = 5120
HQ = 64
KVH = 8
DH = 128
BLK = 64
NSEL = 16
TOK_DEV = 256
GROUP = 8
BATCH = 4
SEQLEN = 512
TILES = 8
N_SEQ = 2


def choose_blocks(key):
    seeded = jax.random.fold_in(key, 17)
    rank_key, order_key = jax.random.split(seeded)
    filler_key = jax.random.fold_in(seeded, 5)
    near_key, far_key, coin_key = jax.random.split(filler_key, 3)
    width_all = TILES + NSEL
    candidate = jnp.arange(width_all, dtype=jnp.int32)[None, None, None, :]
    tile_of = jnp.arange(TILES, dtype=jnp.int32)[None, :, None, None]
    random_part = jax.random.randint(rank_key, (BATCH, TILES, KVH, width_all), 0, 1 << 20)
    ranking = random_part * width_all + candidate
    ranking = jnp.where(candidate <= tile_of, ranking, -1 - candidate)
    ranking = jnp.where(candidate == 0, 1 << 30, ranking)
    ranking = jnp.where(candidate == tile_of, (1 << 30) + 1, ranking)
    best_scores, best_slots = lax.top_k(ranking, NSEL)
    usable = (best_scores >= 0).astype(jnp.int32)
    chosen = (best_slots % TILES).astype(jnp.int32)
    shuffle_keys = jax.random.randint(order_key, (BATCH, TILES, KVH, NSEL), 0, 1 << 20) * NSEL + jnp.arange(NSEL, dtype=jnp.int32)
    shuffle = jnp.argsort(shuffle_keys, axis=-1)
    chosen = jnp.take_along_axis(chosen, shuffle, axis=-1)
    usable = jnp.take_along_axis(usable, shuffle, axis=-1)
    slot_shape = (BATCH, TILES, KVH, NSEL)
    near = jax.random.randint(near_key, slot_shape, 0, 1 << 20) % (tile_of + 1)
    far = jax.random.randint(far_key, slot_shape, 0, TILES)
    coin = jax.random.randint(coin_key, slot_shape, 0, 2)
    filler = jnp.where(coin == 0, near, far).astype(jnp.int32)
    chosen = jnp.where(usable > 0, chosen, filler).astype(jnp.int32)
    return (chosen, usable)


def draw_block_ids(key, part):
    return choose_blocks(key)[0]


def draw_block_valid(key, part):
    return choose_blocks(key)[1]


def block_scale(key, dims, cuts, smallest, largest):
    loudness = 1.0
    for position, blocks in cuts:
        heights = jax.random.uniform(jax.random.fold_in(jax.random.fold_in(key, 6), position), (blocks,), jnp.float32, smallest / len(cuts), largest / len(cuts))
        loudness = loudness * jnp.repeat(jnp.exp(heights), dims[position] // blocks).reshape((-1,) + (1,) * (len(dims) - 1 - position))
    return loudness


def bell_draw(rng, extent, spread, limit, cuts=(), kind=jnp.bfloat16):
    drawn = jax.random.normal(rng, extent, jnp.float32) * spread
    if len(cuts) > 0:
        drawn = block_scale(rng, extent, cuts, -0.22, 0.18) * drawn
    return jnp.clip(drawn, min=-limit, max=limit).astype(kind)


def setup_inputs(seed: int = 0) -> dict:
    splits = jax.random.split(jax.random.key(seed), 11)
    return {
        "queries": bell_draw(splits[0], (BATCH, SEQLEN, HQ, DH), 1.0, 6.0, ((0, 4), (1, 2), (2, 4))),
        "keys": bell_draw(splits[1], (BATCH, SEQLEN, KVH, DH), 1.0, 6.0, ((0, 4), (1, 2), (2, 4))),
        "values": bell_draw(splits[2], (BATCH, SEQLEN, KVH, DH), 1.0, 6.0, ((0, 4), (1, 2), (2, 4))),
        "attn_out": bell_draw(splits[3], (BATCH, SEQLEN, HQ, DH), 1.0, 6.0, ((0, 4), (1, 2), (2, 4))),
        "out_grad": bell_draw(splits[4], (BATCH, SEQLEN, HQ, DH), 1.0, 6.0, ((0, 4), (1, 2), (2, 4))),
        "gate_values": jnp.clip(0.05 + 0.9 * jax.random.uniform(splits[5], (BATCH, HQ, SEQLEN), jnp.float32) ** block_scale(splits[5], (BATCH, HQ, SEQLEN), ((0, 4), (1, 4), (2, 2)), -0.2, 0.2), 0.05, 0.95),
        "log_totals": jnp.clip(3.0 + 2.0 * jax.random.uniform(splits[6], (BATCH, HQ, SEQLEN), jnp.float32) ** block_scale(splits[6], (BATCH, HQ, SEQLEN), ((0, 4), (1, 4), (2, 2)), -0.2, 0.2), 3.0, 5.0),
        "hidden": bell_draw(splits[7], (BATCH, SEQLEN, D), 1.0, 6.0, ((0, 4), (1, 2), (2, 4))),
        "block_ids": draw_block_ids(jax.random.fold_in(splits[10], 71), 0),
        "block_valid": draw_block_valid(jax.random.fold_in(splits[10], 71), 0),
    }


def reference(queries, keys, values, attn_out, out_grad, gate_values, log_totals, hidden, block_ids, block_valid):
    factor = DH ** -0.5
    tiles_dev = TOK_DEV // BLK
    key_blocks = keys.reshape(BATCH, TILES, BLK, KVH, DH)
    value_blocks = values.reshape(BATCH, TILES, BLK, KVH, DH)
    batch_index = jnp.arange(BATCH, dtype=jnp.int32)[:, None, None]
    kv_index = jnp.arange(KVH, dtype=jnp.int32)[None, :, None]
    offsets = jnp.arange(BLK, dtype=jnp.int32)

    def tile_step(partial_value, tile_index):
        first_row = tile_index * BLK
        query_tile = lax.dynamic_slice_in_dim(queries, first_row, BLK, 1).reshape(BATCH, BLK, KVH, GROUP, DH).astype(jnp.float32)
        output_tile = lax.dynamic_slice_in_dim(attn_out, first_row, BLK, 1).reshape(BATCH, BLK, KVH, GROUP, DH).astype(jnp.float32)
        upstream = lax.dynamic_slice_in_dim(out_grad, first_row, BLK, 1).reshape(BATCH, BLK, KVH, GROUP, DH).astype(jnp.float32)
        gate_tile = lax.dynamic_slice_in_dim(gate_values, first_row, BLK, 2).reshape(BATCH, KVH, GROUP, BLK)
        totals = lax.dynamic_slice_in_dim(log_totals, first_row, BLK, 2).reshape(BATCH, KVH, GROUP, BLK)
        chosen = lax.dynamic_index_in_dim(block_ids, tile_index, 1, keepdims=False)
        usable = lax.dynamic_index_in_dim(block_valid, tile_index, 1, keepdims=False) > 0
        key_sel = key_blocks[batch_index, chosen, :, kv_index, :].astype(jnp.float32)
        value_sel = value_blocks[batch_index, chosen, :, kv_index, :].astype(jnp.float32)
        gates_by_row = jnp.transpose(gate_tile, (0, 3, 1, 2))
        grad_low = lax.optimization_barrier((gates_by_row[..., None] * upstream).astype(jnp.bfloat16))
        grad_output = grad_low.astype(jnp.float32)
        row_delta = jnp.transpose(jnp.sum(grad_output * output_tile, axis=-1), (0, 2, 3, 1))
        gate_grad = jnp.sum(upstream * output_tile, axis=-1)
        logit_grad = (gate_grad * gates_by_row * (1.0 - gates_by_row)).astype(jnp.bfloat16)
        scores = jnp.einsum("bikgd,bknjd->bkginj", query_tile, key_sel) * factor
        query_pos = first_row + offsets
        key_pos = chosen[..., None] * BLK + offsets
        allowed = usable[:, :, None, :, None] & (key_pos[:, :, None, :, :] <= query_pos[None, None, :, None, None])
        probability = jnp.where(allowed[:, :, None], jnp.exp(scores - totals[..., None, None]), 0.0)
        prob_grad = jnp.einsum("bikgd,bknjd->bkginj", grad_output, value_sel)
        dscore = lax.optimization_barrier((probability * (prob_grad - row_delta[..., None, None])).astype(jnp.bfloat16)).astype(jnp.float32)
        prob_low = lax.optimization_barrier(probability.astype(jnp.bfloat16)).astype(jnp.float32)
        query_part = (jnp.einsum("bkginj,bknjd->bikgd", dscore, key_sel) * factor).astype(jnp.bfloat16)
        key_part = jnp.einsum("bkginj,bikgd->bknjd", dscore, query_tile) * factor
        value_part = jnp.einsum("bkginj,bikgd->bknjd", prob_low, grad_output)
        partial_value = partial_value.at[batch_index, chosen, :, kv_index, :].add(jnp.concatenate([key_part, value_part], axis=-1))
        return partial_value, (query_part, logit_grad)

    def source_step(total, source):
        tile_ids = source * tiles_dev + jnp.arange(tiles_dev, dtype=jnp.int32)
        fresh = jnp.zeros((BATCH, TILES, BLK, KVH, 2 * DH), jnp.float32)
        partial_value, parts = lax.scan(tile_step, fresh, tile_ids)
        rounded = lax.optimization_barrier(partial_value.astype(jnp.bfloat16)).astype(jnp.float32)
        return total + rounded, parts

    start_total = jnp.zeros((BATCH, TILES, BLK, KVH, 2 * DH), jnp.float32)
    summed_all, (query_parts, logit_parts) = lax.scan(source_step, start_total, jnp.arange(N_SEQ, dtype=jnp.int32))
    query_parts = query_parts.reshape((TILES,) + query_parts.shape[2:])
    logit_parts = logit_parts.reshape((TILES,) + logit_parts.shape[2:])
    query_grad = jnp.swapaxes(query_parts, 0, 1).reshape(BATCH, SEQLEN, HQ, DH)
    logit_rows = jnp.transpose(logit_parts.reshape(TILES, BATCH, BLK, HQ), (3, 1, 0, 2)).reshape(HQ, BATCH * SEQLEN)
    gate_weight_grad = jnp.dot(logit_rows, hidden.reshape(BATCH * SEQLEN, D), preferred_element_type=jnp.float32) * (1.0 / (BATCH * SEQLEN) ** 0.5)
    summed = summed_all.reshape(BATCH, SEQLEN, KVH, 2 * DH)
    return query_grad, summed[..., :DH].astype(jnp.bfloat16), summed[..., DH:].astype(jnp.bfloat16), gate_weight_grad
```

```python
import functools
import math

import jax
import jax.numpy as jnp
from jax import lax
from jax.experimental import pallas as pl
from jax.experimental.pallas import tpu as pltpu
from jax.sharding import PartitionSpec as P

F32 = jnp.float32
BF16 = jnp.bfloat16
MASKED = -1e9
NT = (((1,), (1,)), ((), ()))
NN = (((1,), (0,)), ((), ()))
TN = (((0,), (0,)), ((), ()))


def mm(a, b, dims):
    return lax.dot_general(a, b, dims, preferred_element_type=F32)


def split3(x):
    hi = x.astype(BF16).astype(F32)
    mid = (x - hi).astype(BF16).astype(F32)
    lo = (x - hi - mid).astype(BF16).astype(F32)
    return hi, mid, lo


def kernel(
    dims,
    ids_ref, valid_ref, q_ref, ao_ref, og_ref, gate_ref, tot_ref, hid_ref, kv_ref,
    qg_ref, dkv_ref, wg_ref,
    cols, lgt, qaug, doaug, dq_acc, kv_in, kv_acc, g_send, g_recv,
    lg_all, w_own, w_send, w_recv, x_all, o_all,
    kv_ss, kv_rs, g_ss, g_rs, lg_ss, lg_rs, w_ss, w_rs, x_ss, x_rs, o_ss, o_rs,
):
    n_seq, n_head, n_dp, tiles, blk, kvh, group, dh, nsel = dims
    heads = kvh * group
    rows = blk * group
    toks = tiles * blk
    s = lax.axis_index("seq")
    h = lax.axis_index("head")
    d = lax.axis_index("dp")
    root = math.sqrt(dh)
    cexp = math.log2(math.e) / root

    barrier = pltpu.get_barrier_semaphore()
    for name, me, n in (("seq", s, n_seq), ("head", h, n_head), ("dp", d, n_dp)):
        for off in range(1, n):
            pl.semaphore_signal(
                barrier, inc=1, device_id={name: lax.rem(me + off, n)},
                device_id_type=pl.DeviceIdType.MESH)
    pl.semaphore_wait(barrier, n_seq + n_head + n_dp - 3)

    def kv_copy(k, src_s, dst_s):
        return pltpu.make_async_remote_copy(
            src_ref=kv_ref.at[k], dst_ref=kv_in.at[src_s, k],
            send_sem=kv_ss.at[dst_s, k], recv_sem=kv_rs.at[src_s, k],
            device_id={"seq": dst_s}, device_id_type=pl.DeviceIdType.MESH)

    def g_copy(k, src_s, dst_s):
        return pltpu.make_async_remote_copy(
            src_ref=g_send.at[dst_s, k], dst_ref=g_recv.at[src_s, k],
            send_sem=g_ss.at[dst_s, k], recv_sem=g_rs.at[src_s, k],
            device_id={"seq": dst_s}, device_id_type=pl.DeviceIdType.MESH)

    def slot_copy(src, dst, ss, rs, axis, src_i, dst_i):
        return pltpu.make_async_remote_copy(
            src_ref=src, dst_ref=dst.at[src_i],
            send_sem=ss.at[dst_i], recv_sem=rs.at[src_i],
            device_id={axis: dst_i}, device_id_type=pl.DeviceIdType.MESH)

    def loop(lo, hi, fn):
        def step(i, c):
            fn(i)
            return c
        lax.fori_loop(lo, hi, step, 0)

    for k in range(kvh):
        loop(s + 1, n_seq, lambda j: kv_copy(k, s, j).start())

    hi, mid, lo = split3(tot_ref[...] * (-root))
    stack = jnp.concatenate(
        [gate_ref[...], hi, mid, lo, jnp.zeros((128 - 4 * heads, toks), F32)], axis=0)
    cols[...] = jnp.transpose(stack)

    lane = lax.broadcasted_iota(jnp.int32, (rows, 128), 1)
    g_of = lax.rem(lax.broadcasted_iota(jnp.int32, (rows, 128), 0), group)
    pick = (
        lax.broadcasted_iota(jnp.int32, (blk, rows), 0)
        == lax.broadcasted_iota(jnp.int32, (blk, rows), 1) // group
    ).astype(BF16)
    lane1 = lax.broadcasted_iota(jnp.int32, (1, 128), 1)

    def prep(t):
        at = pl.ds(pl.multiple_of(t * blk, blk), blk)
        og = og_ref[at].astype(F32)
        ao = ao_ref[at].astype(F32)
        q = q_ref[at].astype(F32)
        wide = jnp.broadcast_to(cols[at][:, None, :], (blk, group, 128)).reshape(rows, 128)
        x = jnp.zeros((rows, 128), F32)
        for k in range(kvh):
            part = slice(k * group, (k + 1) * group)
            ogk = og[:, part, :].reshape(rows, dh)
            aok = ao[:, part, :].reshape(rows, dh)
            qk = q[:, part, :].reshape(rows, dh)
            mine = lax.rem(lane, heads) == g_of + k * group
            sel = jnp.full((1, 128), MASKED, F32)
            for n in range(nsel):
                b = jnp.where(valid_ref[t, k, n] > 0, ids_ref[t, k, n], -1000)
                sel = jnp.where(lane1 == b + 4 * heads, 0.0, sel)
            gate = jnp.sum(jnp.where(mine & (lane < heads), wide, 0.0), axis=1, keepdims=True)
            tail = jnp.where(
                lane >= 4 * heads, sel, jnp.where(mine & (lane >= heads), wide, 0.0))
            qaug[t, k, :, :dh] = qk.astype(BF16)
            qaug[t, k, :, dh:] = tail.astype(BF16)
            go = (gate * ogk).astype(BF16)
            dl_hi, dl_mid, dl_lo = split3(
                -jnp.sum(go.astype(F32) * aok, axis=1, keepdims=True))
            doaug[t, k, :, :dh] = go
            doaug[t, k, :, dh:] = jnp.where(
                lane == heads, dl_hi,
                jnp.where(lane == heads + 1, dl_mid,
                          jnp.where(lane == heads + 2, dl_lo, 0.0))).astype(BF16)
            lg = jnp.sum(ogk * aok, axis=1, keepdims=True) * gate * (1.0 - gate)
            x = x + jnp.where(lane == g_of + k * group, lg, 0.0)
        lgt[at, :] = mm(pick, x.astype(BF16), NN)

    loop(0, tiles, prep)
    lg_all[h] = jnp.transpose(lgt[...])[:heads].astype(BF16)
    for off in range(1, n_head):
        slot_copy(lg_all.at[h], lg_all, lg_ss, lg_rs, "head", h, lax.rem(h + off, n_head)).start()

    def key_tail(r):
        ln = lax.broadcasted_iota(jnp.int32, (toks, 128), 1)
        bk = lax.broadcasted_iota(jnp.int32, (toks, 128), 0) // blk + r * tiles
        hot = (ln == bk + 4 * heads) | ((ln >= heads) & (ln < 4 * heads))
        return jnp.where(hot, 1.0, 0.0).astype(BF16)

    def pair(kk, vv, tail, t, k, causal):
        nk = kk.shape[0]
        qa = qaug[t, k]
        da = doaug[t, k]
        sc = mm(jnp.concatenate([kk, tail], axis=1), qa, NT)
        p = jnp.exp2(sc * cexp)
        if causal:
            row = lax.broadcasted_iota(jnp.int32, (nk, rows), 0) - (nk - blk)
            tok = lax.broadcasted_iota(jnp.int32, (nk, rows), 1) // group
            p = jnp.where(row <= tok, p, 0.0)
        dp = mm(jnp.concatenate([vv, tail], axis=1), da, NT)
        ds = (p * dp).astype(BF16)
        dq = mm(ds, kk, TN)
        dk = mm(ds, qa[:, :dh], NN)
        dv = mm(p.astype(BF16), da[:, :dh], NN)
        return dq, dk, dv

    own_tail = key_tail(s)

    def local(k):
        for t in range(tiles - 1, -1, -1):
            nk = (t + 1) * blk
            dq, dk, dv = pair(kv_ref[k, 0, :nk], kv_ref[k, 1, :nk], own_tail[:nk], t, k, True)
            dq_acc[t, k] = dq
            if t == tiles - 1:
                kv_acc[k, 0] = dk
                kv_acc[k, 1] = dv
            else:
                kv_acc[k, 0, :nk] += dk
                kv_acc[k, 1, :nk] += dv

    def remote(k):
        def one(i):
            r = s - 1 - i
            kv_copy(k, r, s).wait_recv()
            tail = key_tail(r)
            kk = kv_in[r, k, 0]
            vv = kv_in[r, k, 1]
            dks = dvs = None
            for t in range(tiles):
                dq, dk, dv = pair(kk, vv, tail, t, k, False)
                dq_acc[t, k] += dq
                dks = dk if dks is None else dks + dk
                dvs = dv if dvs is None else dvs + dv
            g_send[r, k, 0] = (dks * (1.0 / root)).astype(BF16)
            g_send[r, k, 1] = dvs.astype(BF16)
            g_copy(k, s, r).start()
        loop(0, s, one)

    for k in range(kvh):
        local(k)

    for off in range(1, n_head):
        j = lax.rem(h + off, n_head)
        slot_copy(lg_all.at[j], lg_all, lg_ss, lg_rs, "head", j, h).wait_recv()
    hq = n_head * heads
    w = mm(lg_all[...].reshape(hq, toks), hid_ref[...], NN)
    part = hq // n_dp
    for j in range(n_dp):
        w_own[j] = w[j * part:(j + 1) * part]
        w_send[j] = w[j * part:(j + 1) * part].astype(BF16)
    for off in range(1, n_dp):
        j = lax.rem(d + off, n_dp)
        slot_copy(w_send.at[j], w_recv, w_ss, w_rs, "dp", d, j).start()

    remote(0)

    total = w_own[d]
    for off in range(1, n_dp):
        j = lax.rem(d + off, n_dp)
        slot_copy(w_send.at[d], w_recv, w_ss, w_rs, "dp", j, d).wait_recv()
        total = total + w_recv[j].astype(F32)
    x_all[s] = total.astype(BF16)
    for off in range(1, n_seq):
        slot_copy(x_all.at[s], x_all, x_ss, x_rs, "seq", s, lax.rem(s + off, n_seq)).start()

    for k in range(1, kvh):
        remote(k)

    for off in range(1, n_seq):
        j = lax.rem(s + off, n_seq)
        slot_copy(x_all.at[j], x_all, x_ss, x_rs, "seq", j, s).wait_recv()
    total = x_all[0].astype(F32)
    for j in range(1, n_seq):
        total = total + x_all[j].astype(F32)
    o_all[d] = (total * (1.0 / math.sqrt(n_dp * n_seq * toks))).astype(BF16)
    for off in range(1, n_dp):
        slot_copy(o_all.at[d], o_all, o_ss, o_rs, "dp", d, lax.rem(d + off, n_dp)).start()

    for t in range(tiles):
        qg_ref[t * blk:(t + 1) * blk] = jnp.concatenate(
            [dq_acc[t, k].reshape(blk, group, dh) for k in range(kvh)], axis=1
        ).__mul__(1.0 / root).astype(BF16)

    for k in range(kvh):
        kv_acc[k, 0] = (kv_acc[k, 0] * (1.0 / root)).astype(BF16).astype(F32)
        kv_acc[k, 1] = kv_acc[k, 1].astype(BF16).astype(F32)

        def add(j, k=k):
            g_copy(k, j, s).wait_recv()
            kv_acc[k] += g_recv[j, k].astype(F32)
        loop(s + 1, n_seq, add)
        dkv_ref[k] = kv_acc[k].astype(BF16)

    for off in range(1, n_dp):
        j = lax.rem(d + off, n_dp)
        slot_copy(o_all.at[j], o_all, o_ss, o_rs, "dp", j, d).wait_recv()
    for j in range(n_dp):
        wg_ref[j * part:(j + 1) * part] = o_all[j].astype(F32)

    for k in range(kvh):
        loop(s + 1, n_seq, lambda j: kv_copy(k, s, j).wait_send())
        loop(0, s, lambda j: g_copy(k, s, j).wait_send())
    for off in range(1, n_head):
        slot_copy(lg_all.at[h], lg_all, lg_ss, lg_rs, "head", h, lax.rem(h + off, n_head)).wait_send()
    for off in range(1, n_dp):
        j = lax.rem(d + off, n_dp)
        slot_copy(w_send.at[j], w_recv, w_ss, w_rs, "dp", d, j).wait_send()
        slot_copy(o_all.at[d], o_all, o_ss, o_rs, "dp", d, j).wait_send()
    for off in range(1, n_seq):
        slot_copy(x_all.at[s], x_all, x_ss, x_rs, "seq", s, lax.rem(s + off, n_seq)).wait_send()


def on_device(
    queries, keys, values, attn_out, out_grad, gate_values, log_totals, hidden,
    block_ids, block_valid,
):
    toks, heads, dh = queries.shape[1:]
    kvh = keys.shape[2]
    tiles, nsel = block_ids.shape[1], block_ids.shape[3]
    group = heads // kvh
    blk = toks // tiles
    rows = blk * group
    n_seq, n_head, n_dp = (lax.axis_size(a) for a in ("seq", "head", "dp"))
    hq = n_head * heads
    width = hidden.shape[2]
    part = hq // n_dp
    dims = (n_seq, n_head, n_dp, tiles, blk, kvh, group, dh, nsel)
    kv = jnp.transpose(jnp.stack([keys[0], values[0]]), (2, 0, 1, 3))
    vm = pl.BlockSpec(memory_space=pltpu.VMEM)
    sm = pl.BlockSpec(memory_space=pltpu.SMEM)
    dma = pltpu.SemaphoreType.DMA
    qg, dkv, wg = pl.pallas_call(
        functools.partial(kernel, dims),
        out_shape=(
            jax.ShapeDtypeStruct((toks, heads, dh), BF16),
            jax.ShapeDtypeStruct((kvh, 2, toks, dh), BF16),
            jax.ShapeDtypeStruct((hq, width), F32),
        ),
        in_specs=[sm, sm] + [vm] * 7,
        out_specs=(vm, vm, vm),
        scratch_shapes=[
            pltpu.VMEM((toks, 128), F32),
            pltpu.VMEM((toks, 128), F32),
            pltpu.VMEM((tiles, kvh, rows, 2 * dh), BF16),
            pltpu.VMEM((tiles, kvh, rows, 2 * dh), BF16),
            pltpu.VMEM((tiles, kvh, rows, dh), F32),
            pltpu.VMEM((n_seq, kvh, 2, toks, dh), BF16),
            pltpu.VMEM((kvh, 2, toks, dh), F32),
            pltpu.VMEM((n_seq, kvh, 2, toks, dh), BF16),
            pltpu.VMEM((n_seq, kvh, 2, toks, dh), BF16),
            pltpu.VMEM((n_head, heads, toks), BF16),
            pltpu.VMEM((n_dp, part, width), F32),
            pltpu.VMEM((n_dp, part, width), BF16),
            pltpu.VMEM((n_dp, part, width), BF16),
            pltpu.VMEM((n_seq, part, width), BF16),
            pltpu.VMEM((n_dp, part, width), BF16),
            dma((n_seq, kvh)), dma((n_seq, kvh)), dma((n_seq, kvh)), dma((n_seq, kvh)),
            dma((n_head,)), dma((n_head,)), dma((n_dp,)), dma((n_dp,)),
            dma((n_seq,)), dma((n_seq,)), dma((n_dp,)), dma((n_dp,)),
        ],
        compiler_params=pltpu.CompilerParams(
            collective_id=0, has_side_effects=True, vmem_limit_bytes=60 * 1024 * 1024),
        name="attention_backward",
    )(block_ids[0], block_valid[0], queries[0], attn_out[0], out_grad[0],
      gate_values[0], log_totals[0], hidden[0], kv)
    key_grad = jnp.transpose(dkv[:, 0], (1, 0, 2))[None]
    value_grad = jnp.transpose(dkv[:, 1], (1, 0, 2))[None]
    return qg[None], key_grad, value_grad, wg


def solution(mesh):
    return jax.shard_map(
        on_device,
        mesh=mesh,
        in_specs=(
            P("dp", "seq", "head", None),
            P("dp", "seq", "head", None),
            P("dp", "seq", "head", None),
            P("dp", "seq", "head", None),
            P("dp", "seq", "head", None),
            P("dp", "head", "seq"),
            P("dp", "head", "seq"),
            P("dp", "seq", "head"),
            P("dp", "seq", "head", None),
            P("dp", "seq", "head", None),
        ),
        out_specs=(
            P("dp", "seq", "head", None),
            P("dp", "seq", "head", None),
            P("dp", "seq", "head", None),
            P(None, "head"),
        ),
        check_vma=False,
    )
```

```python
import functools
import math

import jax
import jax.numpy as jnp
from jax import lax
from jax.experimental import pallas as pl
from jax.experimental.pallas import tpu as pltpu
from jax.sharding import PartitionSpec as P

F32 = jnp.float32
BF16 = jnp.bfloat16
MASKED = -1e9
NT = (((1,), (1,)), ((), ()))
NN = (((1,), (0,)), ((), ()))
TN = (((0,), (0,)), ((), ()))


def mm(a, b, dims):
    return lax.dot_general(a, b, dims, preferred_element_type=F32)


def split3(x):
    hi = x.astype(BF16).astype(F32)
    mid = (x - hi).astype(BF16).astype(F32)
    lo = (x - hi - mid).astype(BF16).astype(F32)
    return hi, mid, lo


def kernel(
    dims,
    ids_ref, valid_ref, q_hbm, ao_hbm, og_hbm, hid_hbm, gate_ref, tot_ref, k_ref, v_ref,
    qg_hbm, dk_ref, dv_ref, wg_ref,
    q_ref, ao_ref, og_ref, hid_ref, qg_ref, in_s, hid_s, qg_s, cols, lgt, qaug, doaug, dq_acc, kv_in, kv_acc, g_send, g_recv,
    lg_all, w_own, w_send, w_recv, x_all, o_all,
    kv_ss, kv_rs, g_ss, g_rs, lg_ss, lg_rs, w_ss, w_rs, x_ss, x_rs, o_ss, o_rs,
):
    n_seq, n_head, n_dp, tiles, blk, kvh, group, dh, nsel = dims
    heads = kvh * group
    rows = blk * group
    toks = tiles * blk
    s = lax.axis_index("seq")
    h = lax.axis_index("head")
    d = lax.axis_index("dp")
    root = math.sqrt(dh)
    cexp = math.log2(math.e) / root

    def fetch(i, t):
        src, dst = ((og_hbm, og_ref), (ao_hbm, ao_ref), (q_hbm, q_ref))[i]
        at = pl.ds(t * blk, blk)
        return pltpu.make_async_copy(src.at[at], dst.at[at], in_s.at[i, t])

    hid_copy = pltpu.make_async_copy(hid_hbm, hid_ref, hid_s)

    def put(t):
        at = pl.ds(t * blk, blk)
        return pltpu.make_async_copy(qg_ref.at[at], qg_hbm.at[at], qg_s.at[t])

    barrier = pltpu.get_barrier_semaphore()
    for name, me, n in (("seq", s, n_seq), ("head", h, n_head), ("dp", d, n_dp)):
        for off in range(1, n):
            pl.semaphore_signal(
                barrier, inc=1, device_id={name: lax.rem(me + off, n)},
                device_id_type=pl.DeviceIdType.MESH)
    for t in range(tiles):
        for i in range(3):
            fetch(i, t).start()
    hid_copy.start()
    pl.semaphore_wait(barrier, n_seq + n_head + n_dp - 3)

    def kv_copy(k, c, src_s, dst_s):
        return pltpu.make_async_remote_copy(
            src_ref=(k_ref, v_ref)[c].at[k], dst_ref=kv_in.at[src_s, k, c],
            send_sem=kv_ss.at[dst_s, k, c], recv_sem=kv_rs.at[src_s, k, c],
            device_id={"seq": dst_s}, device_id_type=pl.DeviceIdType.MESH)

    def g_copy(k, src_s, dst_s):
        return pltpu.make_async_remote_copy(
            src_ref=g_send.at[dst_s, k], dst_ref=g_recv.at[src_s, k],
            send_sem=g_ss.at[dst_s, k], recv_sem=g_rs.at[src_s, k],
            device_id={"seq": dst_s}, device_id_type=pl.DeviceIdType.MESH)

    def slot_copy(src, dst, ss, rs, axis, src_i, dst_i):
        return pltpu.make_async_remote_copy(
            src_ref=src, dst_ref=dst.at[src_i],
            send_sem=ss.at[dst_i], recv_sem=rs.at[src_i],
            device_id={axis: dst_i}, device_id_type=pl.DeviceIdType.MESH)

    def loop(lo, hi, fn):
        def step(i, c):
            fn(i)
            return c
        lax.fori_loop(lo, hi, step, 0)

    for k in range(kvh):
        for c in range(2):
            loop(s + 1, n_seq, lambda j: kv_copy(k, c, s, j).start())

    hi, mid, lo = split3(tot_ref[...] * (-root))
    stack = jnp.concatenate(
        [gate_ref[...], hi, mid, lo, jnp.zeros((128 - 4 * heads, toks), F32)], axis=0)
    cols[...] = jnp.transpose(stack)

    lane = lax.broadcasted_iota(jnp.int32, (1, group, 128), 2)
    g_of = lax.broadcasted_iota(jnp.int32, (1, group, 128), 1)
    pick = (
        lax.broadcasted_iota(jnp.int32, (blk, rows), 0)
        == lax.broadcasted_iota(jnp.int32, (blk, rows), 1) // group
    ).astype(BF16)

    def prep(t):
        at = pl.ds(pl.multiple_of(t * blk, blk), blk)
        for i in range(3):
            fetch(i, t).wait()
        og = og_ref[at].astype(F32)
        ao = ao_ref[at].astype(F32)
        q = q_ref[at].astype(F32)
        wide = jnp.broadcast_to(cols[at][:, None, :], (blk, group, 128))
        x = jnp.zeros((blk, group, 128), F32)
        for k in range(kvh):
            part = slice(k * group, (k + 1) * group)
            ogk, aok, qk = og[:, part, :], ao[:, part, :], q[:, part, :]
            head = g_of + k * group
            mine = lax.rem(lane, heads) == head
            sel = jnp.full((1, group, 128), MASKED, F32)
            for n in range(nsel):
                b = jnp.where(valid_ref[t, k, n] > 0, ids_ref[t, k, n], -1000)
                sel = jnp.where(lane == b + 4 * heads, 0.0, sel)
            gate = jnp.sum(jnp.where(lane == head, wide, 0.0), axis=2, keepdims=True)
            tail = jnp.where(
                lane >= 4 * heads, sel, jnp.where(mine & (lane >= heads), wide, 0.0))
            qaug[t, k, :, :dh] = qk.reshape(rows, dh).astype(BF16)
            qaug[t, k, :, dh:] = tail.reshape(rows, 128).astype(BF16)
            go = (gate * ogk).reshape(rows, dh).astype(BF16)
            wide_go = go.astype(F32).reshape(blk, group, dh)
            dl_hi, dl_mid, dl_lo = split3(-jnp.sum(wide_go * aok, axis=2, keepdims=True))
            doaug[t, k, :, :dh] = go
            doaug[t, k, :, dh:] = jnp.where(
                lane == heads, dl_hi,
                jnp.where(lane == heads + 1, dl_mid,
                          jnp.where(lane == heads + 2, dl_lo, 0.0))
            ).reshape(rows, 128).astype(BF16)
            lg = jnp.sum(ogk * aok, axis=2, keepdims=True) * gate * (1.0 - gate)
            x = x + jnp.where(lane == head, lg, 0.0)
            if k > 0:
                dq_acc[t, k] = jnp.zeros((rows, dh), F32)
        lgt[at, :] = mm(pick, x.reshape(rows, 128).astype(BF16), NN)

    loop(0, tiles, prep)
    lg_all[h] = jnp.transpose(lgt[...])[:heads].astype(BF16)
    for off in range(1, n_head):
        slot_copy(lg_all.at[h], lg_all, lg_ss, lg_rs, "head", h, lax.rem(h + off, n_head)).start()

    def key_tail(r):
        ln = lax.broadcasted_iota(jnp.int32, (toks, 128), 1)
        bk = lax.broadcasted_iota(jnp.int32, (toks, 128), 0) // blk + r * tiles
        hot = (ln == bk + 4 * heads) | ((ln >= heads) & (ln < 4 * heads))
        return jnp.where(hot, 1.0, 0.0).astype(BF16)

    def pair(kk, vv, tail, t, k, causal):
        nk = kk.shape[0]
        qa = qaug[t, k]
        da = doaug[t, k]
        sc = mm(jnp.concatenate([kk, tail], axis=1), qa, NT)
        p = jnp.exp2(sc * cexp)
        if causal:
            row = lax.broadcasted_iota(jnp.int32, (nk, rows), 0) - (nk - blk)
            tok = lax.broadcasted_iota(jnp.int32, (nk, rows), 1) // group
            p = jnp.where(row <= tok, p, 0.0)
        dp = mm(jnp.concatenate([vv, tail], axis=1), da, NT)
        ds = (p * dp).astype(BF16)
        dq = mm(ds, kk, TN)
        dk = mm(ds, qa[:, :dh], NN)
        dv = mm(p.astype(BF16), da[:, :dh], NN)
        return dq, dk, dv

    own_tail = key_tail(s)

    def local(k):
        for t in range(tiles - 1, -1, -1):
            nk = (t + 1) * blk
            dq, dk, dv = pair(k_ref[k, :nk], v_ref[k, :nk], own_tail[:nk], t, k, True)
            if k == 0:
                dq_acc[t, k] = dq
            else:
                dq_acc[t, k] += dq
            if t == tiles - 1:
                kv_acc[k, 0] = dk
                kv_acc[k, 1] = dv
            else:
                kv_acc[k, 0, :nk] += dk
                kv_acc[k, 1, :nk] += dv

    def remote(k):
        def one(i):
            r = s - 1 - i
            for c in range(2):
                kv_copy(k, c, r, s).wait_recv()
            tail = key_tail(r)
            kk = kv_in[r, k, 0]
            vv = kv_in[r, k, 1]
            dks = dvs = None
            for t in range(tiles):
                dq, dk, dv = pair(kk, vv, tail, t, k, False)
                dq_acc[t, k] += dq
                dks = dk if dks is None else dks + dk
                dvs = dv if dvs is None else dvs + dv
            g_send[r, k, 0] = (dks * (1.0 / root)).astype(BF16)
            g_send[r, k, 1] = dvs.astype(BF16)
            g_copy(k, s, r).start()
        loop(0, s, one)

    local(0)

    for off in range(1, n_head):
        j = lax.rem(h + off, n_head)
        slot_copy(lg_all.at[j], lg_all, lg_ss, lg_rs, "head", j, h).wait_recv()
    hid_copy.wait()
    hq = n_head * heads
    w = mm(lg_all[...].reshape(hq, toks), hid_ref[...], NN)
    part = hq // n_dp
    for j in range(n_dp):
        w_own[j] = w[j * part:(j + 1) * part]
        w_send[j] = w[j * part:(j + 1) * part].astype(BF16)
    for off in range(1, n_dp):
        j = lax.rem(d + off, n_dp)
        slot_copy(w_send.at[j], w_recv, w_ss, w_rs, "dp", d, j).start()

    remote(0)

    total = w_own[d]
    for off in range(1, n_dp):
        j = lax.rem(d + off, n_dp)
        slot_copy(w_send.at[d], w_recv, w_ss, w_rs, "dp", j, d).wait_recv()
        total = total + w_recv[j].astype(F32)
    x_all[s] = total.astype(BF16)
    for off in range(1, n_seq):
        slot_copy(x_all.at[s], x_all, x_ss, x_rs, "seq", s, lax.rem(s + off, n_seq)).start()

    for k in range(1, kvh):
        remote(k)

    for off in range(1, n_seq):
        j = lax.rem(s + off, n_seq)
        slot_copy(x_all.at[j], x_all, x_ss, x_rs, "seq", j, s).wait_recv()
    total = x_all[0].astype(F32)
    for j in range(1, n_seq):
        total = total + x_all[j].astype(F32)
    o_all[d] = (total * (1.0 / math.sqrt(n_dp * n_seq * toks))).astype(BF16)
    for off in range(1, n_dp):
        slot_copy(o_all.at[d], o_all, o_ss, o_rs, "dp", d, lax.rem(d + off, n_dp)).start()

    for k in range(1, kvh):
        local(k)
    for t in range(tiles):
        qg_ref[t * blk:(t + 1) * blk] = jnp.concatenate(
            [dq_acc[t, k].reshape(blk, group, dh) for k in range(kvh)], axis=1
        ).__mul__(1.0 / root).astype(BF16)
        put(t).start()

    for k in range(kvh):
        kv_acc[k, 0] = (kv_acc[k, 0] * (1.0 / root)).astype(BF16).astype(F32)
        kv_acc[k, 1] = kv_acc[k, 1].astype(BF16).astype(F32)

        def add(j, k=k):
            g_copy(k, j, s).wait_recv()
            kv_acc[k] += g_recv[j, k].astype(F32)
        loop(s + 1, n_seq, add)
        dk_ref[k] = kv_acc[k, 0].astype(BF16)
        dv_ref[k] = kv_acc[k, 1].astype(BF16)

    for off in range(1, n_dp):
        j = lax.rem(d + off, n_dp)
        slot_copy(o_all.at[j], o_all, o_ss, o_rs, "dp", j, d).wait_recv()
    for j in range(n_dp):
        wg_ref[j] = o_all[j]
    for t in range(tiles):
        put(t).wait()

    for k in range(kvh):
        for c in range(2):
            loop(s + 1, n_seq, lambda j: kv_copy(k, c, s, j).wait_send())
        loop(0, s, lambda j: g_copy(k, s, j).wait_send())
    for off in range(1, n_head):
        slot_copy(lg_all.at[h], lg_all, lg_ss, lg_rs, "head", h, lax.rem(h + off, n_head)).wait_send()
    for off in range(1, n_dp):
        j = lax.rem(d + off, n_dp)
        slot_copy(w_send.at[j], w_recv, w_ss, w_rs, "dp", d, j).wait_send()
        slot_copy(o_all.at[d], o_all, o_ss, o_rs, "dp", d, j).wait_send()
    for off in range(1, n_seq):
        slot_copy(x_all.at[s], x_all, x_ss, x_rs, "seq", s, lax.rem(s + off, n_seq)).wait_send()


def on_device(
    queries, keys, values, attn_out, out_grad, gate_values, log_totals, hidden,
    block_ids, block_valid,
):
    toks, heads, dh = queries.shape[1:]
    kvh = keys.shape[2]
    tiles, nsel = block_ids.shape[1], block_ids.shape[3]
    group = heads // kvh
    blk = toks // tiles
    rows = blk * group
    n_seq, n_head, n_dp = (lax.axis_size(a) for a in ("seq", "head", "dp"))
    hq = n_head * heads
    width = hidden.shape[2]
    part = hq // n_dp
    dims = (n_seq, n_head, n_dp, tiles, blk, kvh, group, dh, nsel)
    any_ = pl.BlockSpec(memory_space=pl.ANY)
    vm = pl.BlockSpec(memory_space=pltpu.VMEM)
    sm = pl.BlockSpec(memory_space=pltpu.SMEM)
    dma = pltpu.SemaphoreType.DMA
    qg, dk, dv, wg = pl.pallas_call(
        functools.partial(kernel, dims),
        out_shape=(
            jax.ShapeDtypeStruct((toks, heads, dh), BF16),
            jax.ShapeDtypeStruct((kvh, toks, dh), BF16),
            jax.ShapeDtypeStruct((kvh, toks, dh), BF16),
            jax.ShapeDtypeStruct((n_dp, part, width), BF16),
        ),
        in_specs=[sm, sm] + [any_] * 4 + [vm] * 4,
        out_specs=(any_, vm, vm, vm),
        scratch_shapes=[
            pltpu.VMEM((toks, heads, dh), BF16),
            pltpu.VMEM((toks, heads, dh), BF16),
            pltpu.VMEM((toks, heads, dh), BF16),
            pltpu.VMEM((toks, width), BF16),
            pltpu.VMEM((toks, heads, dh), BF16),
            dma((3, tiles)), dma, dma((tiles,)),
            pltpu.VMEM((toks, 128), F32),
            pltpu.VMEM((toks, 128), F32),
            pltpu.VMEM((tiles, kvh, rows, 2 * dh), BF16),
            pltpu.VMEM((tiles, kvh, rows, 2 * dh), BF16),
            pltpu.VMEM((tiles, kvh, rows, dh), F32),
            pltpu.VMEM((n_seq, kvh, 2, toks, dh), BF16),
            pltpu.VMEM((kvh, 2, toks, dh), F32),
            pltpu.VMEM((n_seq, kvh, 2, toks, dh), BF16),
            pltpu.VMEM((n_seq, kvh, 2, toks, dh), BF16),
            pltpu.VMEM((n_head, heads, toks), BF16),
            pltpu.VMEM((n_dp, part, width), F32),
            pltpu.VMEM((n_dp, part, width), BF16),
            pltpu.VMEM((n_dp, part, width), BF16),
            pltpu.VMEM((n_seq, part, width), BF16),
            pltpu.VMEM((n_dp, part, width), BF16),
            dma((n_seq, kvh, 2)), dma((n_seq, kvh, 2)), dma((n_seq, kvh)), dma((n_seq, kvh)),
            dma((n_head,)), dma((n_head,)), dma((n_dp,)), dma((n_dp,)),
            dma((n_seq,)), dma((n_seq,)), dma((n_dp,)), dma((n_dp,)),
        ],
        compiler_params=pltpu.CompilerParams(
            collective_id=0, has_side_effects=True, vmem_limit_bytes=67043328),
        name="attention_backward",
    )(block_ids[0], block_valid[0], queries[0], attn_out[0], out_grad[0], hidden[0],
      gate_values[0], log_totals[0],
      jnp.transpose(keys[0], (1, 0, 2)), jnp.transpose(values[0], (1, 0, 2)))
    key_grad = jnp.transpose(dk, (1, 0, 2))[None]
    value_grad = jnp.transpose(dv, (1, 0, 2))[None]
    return qg[None], key_grad, value_grad, wg.reshape(hq, width).astype(F32)


def solution(mesh):
    return jax.shard_map(
        on_device,
        mesh=mesh,
        in_specs=(
            P("dp", "seq", "head", None),
            P("dp", "seq", "head", None),
            P("dp", "seq", "head", None),
            P("dp", "seq", "head", None),
            P("dp", "seq", "head", None),
            P("dp", "head", "seq"),
            P("dp", "head", "seq"),
            P("dp", "seq", "head"),
            P("dp", "seq", "head", None),
            P("dp", "seq", "head", None),
        ),
        out_specs=(
            P("dp", "seq", "head", None),
            P("dp", "seq", "head", None),
            P("dp", "seq", "head", None),
            P(None, "head"),
        ),
        check_vma=False,
    )
```

```python
import functools
import math

import jax
import jax.numpy as jnp
from jax import lax
from jax.experimental import pallas as pl
from jax.experimental.pallas import tpu as pltpu
from jax.sharding import PartitionSpec as P

F32 = jnp.float32
BF16 = jnp.bfloat16
MASKED = -1e9
NT = (((1,), (1,)), ((), ()))
NN = (((1,), (0,)), ((), ()))
TN = (((0,), (0,)), ((), ()))


def mm(a, b, dims):
    return lax.dot_general(a, b, dims, preferred_element_type=F32)


def split3(x):
    hi = x.astype(BF16).astype(F32)
    mid = (x - hi).astype(BF16).astype(F32)
    lo = (x - hi - mid).astype(BF16).astype(F32)
    return hi, mid, lo


def kernel(
    dims,
    ids_ref, valid_ref, q_hbm, ao_hbm, og_hbm, hid_hbm, gate_ref, tot_ref, k_raw, v_raw,
    qg_ref, dk_ref, dv_ref, wg_ref,
    q_ref, ao_ref, og_ref, hid_ref, k_ref, v_ref, in_s, hid_s, cols, lgt, qaug, doaug, dq_acc, kv_in, kv_acc, g_send, g_recv,
    lg_all, w_own, w_send, w_recv, x_all, o_all,
    kv_ss, kv_rs, g_ss, g_rs, lg_ss, lg_rs, w_ss, w_rs, x_ss, x_rs, o_ss, o_rs,
):
    n_seq, n_head, n_dp, tiles, blk, kvh, group, dh, nsel = dims
    heads = kvh * group
    rows = blk * group
    toks = tiles * blk
    s = lax.axis_index("seq")
    h = lax.axis_index("head")
    d = lax.axis_index("dp")
    root = math.sqrt(dh)
    cexp = math.log2(math.e) / root

    def fetch(i, t):
        src, dst = ((og_hbm, og_ref), (ao_hbm, ao_ref), (q_hbm, q_ref))[i]
        at = pl.ds(t * blk, blk)
        return pltpu.make_async_copy(src.at[at], dst.at[at], in_s.at[i, t])

    hid_copy = pltpu.make_async_copy(hid_hbm, hid_ref, hid_s)

    barrier = pltpu.get_barrier_semaphore()
    for name, me, n in (("seq", s, n_seq), ("head", h, n_head), ("dp", d, n_dp)):
        for off in range(1, n):
            pl.semaphore_signal(
                barrier, inc=1, device_id={name: lax.rem(me + off, n)},
                device_id_type=pl.DeviceIdType.MESH)
    for t in range(tiles):
        for i in range(3):
            fetch(i, t).start()
    hid_copy.start()
    for raw, ref in ((k_raw, k_ref), (v_raw, v_ref)):
        wide = raw[...].astype(F32)
        for k in range(kvh):
            ref[k] = wide[:, k, :].astype(BF16)
    pl.semaphore_wait(barrier, n_seq + n_head + n_dp - 3)

    def kv_copy(k, c, src_s, dst_s):
        return pltpu.make_async_remote_copy(
            src_ref=(k_ref, v_ref)[c].at[k], dst_ref=kv_in.at[src_s, k, c],
            send_sem=kv_ss.at[dst_s, k, c], recv_sem=kv_rs.at[src_s, k, c],
            device_id={"seq": dst_s}, device_id_type=pl.DeviceIdType.MESH)

    def g_copy(k, src_s, dst_s):
        return pltpu.make_async_remote_copy(
            src_ref=g_send.at[dst_s, k], dst_ref=g_recv.at[src_s, k],
            send_sem=g_ss.at[dst_s, k], recv_sem=g_rs.at[src_s, k],
            device_id={"seq": dst_s}, device_id_type=pl.DeviceIdType.MESH)

    def slot_copy(src, dst, ss, rs, axis, src_i, dst_i):
        return pltpu.make_async_remote_copy(
            src_ref=src, dst_ref=dst.at[src_i],
            send_sem=ss.at[dst_i], recv_sem=rs.at[src_i],
            device_id={axis: dst_i}, device_id_type=pl.DeviceIdType.MESH)

    def loop(lo, hi, fn):
        def step(i, c):
            fn(i)
            return c
        lax.fori_loop(lo, hi, step, 0)

    for k in range(kvh):
        for c in range(2):
            loop(s + 1, n_seq, lambda j: kv_copy(k, c, s, j).start())

    hi, mid, lo = split3(tot_ref[...] * (-root))
    stack = jnp.concatenate(
        [gate_ref[...], hi, mid, lo, jnp.zeros((128 - 4 * heads, toks), F32)], axis=0)
    cols[...] = jnp.transpose(stack)

    lane = lax.broadcasted_iota(jnp.int32, (1, group, 128), 2)
    g_of = lax.broadcasted_iota(jnp.int32, (1, group, 128), 1)
    pick = (
        lax.broadcasted_iota(jnp.int32, (blk, rows), 0)
        == lax.broadcasted_iota(jnp.int32, (blk, rows), 1) // group
    ).astype(BF16)

    def prep(t):
        at = pl.ds(pl.multiple_of(t * blk, blk), blk)
        for i in range(3):
            fetch(i, t).wait()
        og = og_ref[at].astype(F32)
        ao = ao_ref[at].astype(F32)
        q = q_ref[at].astype(F32)
        wide = jnp.broadcast_to(cols[at][:, None, :], (blk, group, 128))
        x = jnp.zeros((blk, group, 128), F32)
        for k in range(kvh):
            part = slice(k * group, (k + 1) * group)
            ogk, aok, qk = og[:, part, :], ao[:, part, :], q[:, part, :]
            head = g_of + k * group
            mine = lax.rem(lane, heads) == head
            sel = jnp.full((1, group, 128), MASKED, F32)
            for n in range(nsel):
                b = jnp.where(valid_ref[t, k, n] > 0, ids_ref[t, k, n], -1000)
                sel = jnp.where(lane == b + 4 * heads, 0.0, sel)
            gate = jnp.sum(jnp.where(lane == head, wide, 0.0), axis=2, keepdims=True)
            tail = jnp.where(
                lane >= 4 * heads, sel, jnp.where(mine & (lane >= heads), wide, 0.0))
            qaug[t, k, :, :dh] = qk.reshape(rows, dh).astype(BF16)
            qaug[t, k, :, dh:] = tail.reshape(rows, 128).astype(BF16)
            go = (gate * ogk).reshape(rows, dh).astype(BF16)
            wide_go = go.astype(F32).reshape(blk, group, dh)
            dl_hi, dl_mid, dl_lo = split3(-jnp.sum(wide_go * aok, axis=2, keepdims=True))
            doaug[t, k, :, :dh] = go
            doaug[t, k, :, dh:] = jnp.where(
                lane == heads, dl_hi,
                jnp.where(lane == heads + 1, dl_mid,
                          jnp.where(lane == heads + 2, dl_lo, 0.0))
            ).reshape(rows, 128).astype(BF16)
            lg = jnp.sum(ogk * aok, axis=2, keepdims=True) * gate * (1.0 - gate)
            x = x + jnp.where(lane == head, lg, 0.0)
            if k > 0:
                dq_acc[t, k] = jnp.zeros((rows, dh), F32)
        lgt[at, :] = mm(pick, x.reshape(rows, 128).astype(BF16), NN)

    loop(0, tiles, prep)
    lg_all[h] = jnp.transpose(lgt[...])[:heads].astype(BF16)
    for off in range(1, n_head):
        slot_copy(lg_all.at[h], lg_all, lg_ss, lg_rs, "head", h, lax.rem(h + off, n_head)).start()

    def key_tail(r):
        ln = lax.broadcasted_iota(jnp.int32, (toks, 128), 1)
        bk = lax.broadcasted_iota(jnp.int32, (toks, 128), 0) // blk + r * tiles
        hot = (ln == bk + 4 * heads) | ((ln >= heads) & (ln < 4 * heads))
        return jnp.where(hot, 1.0, 0.0).astype(BF16)

    def pair(kk, vv, tail, t, k, causal):
        nk = kk.shape[0]
        qa = qaug[t, k]
        da = doaug[t, k]
        sc = mm(jnp.concatenate([kk, tail], axis=1), qa, NT)
        p = jnp.exp2(sc * cexp)
        if causal:
            row = lax.broadcasted_iota(jnp.int32, (nk, rows), 0) - (nk - blk)
            tok = lax.broadcasted_iota(jnp.int32, (nk, rows), 1) // group
            p = jnp.where(row <= tok, p, 0.0)
        dp = mm(jnp.concatenate([vv, tail], axis=1), da, NT)
        ds = (p * dp).astype(BF16)
        dq = mm(ds, kk, TN)
        dk = mm(ds, qa[:, :dh], NN)
        dv = mm(p.astype(BF16), da[:, :dh], NN)
        return dq, dk, dv

    own_tail = key_tail(s)

    def local(k):
        for t in range(tiles - 1, -1, -1):
            nk = (t + 1) * blk
            dq, dk, dv = pair(k_ref[k, :nk], v_ref[k, :nk], own_tail[:nk], t, k, True)
            if k == 0:
                dq_acc[t, k] = dq
            else:
                dq_acc[t, k] += dq
            if t == tiles - 1:
                kv_acc[k, 0] = dk
                kv_acc[k, 1] = dv
            else:
                kv_acc[k, 0, :nk] += dk
                kv_acc[k, 1, :nk] += dv

    def remote(k):
        def one(i):
            r = s - 1 - i
            for c in range(2):
                kv_copy(k, c, r, s).wait_recv()
            tail = key_tail(r)
            kk = kv_in[r, k, 0]
            vv = kv_in[r, k, 1]
            dks = dvs = None
            for t in range(tiles):
                dq, dk, dv = pair(kk, vv, tail, t, k, False)
                dq_acc[t, k] += dq
                dks = dk if dks is None else dks + dk
                dvs = dv if dvs is None else dvs + dv
            g_send[r, k, 0] = (dks * (1.0 / root)).astype(BF16)
            g_send[r, k, 1] = dvs.astype(BF16)
            g_copy(k, s, r).start()
        loop(0, s, one)

    local(0)

    for off in range(1, n_head):
        j = lax.rem(h + off, n_head)
        slot_copy(lg_all.at[j], lg_all, lg_ss, lg_rs, "head", j, h).wait_recv()
    hid_copy.wait()
    hq = n_head * heads
    w = mm(lg_all[...].reshape(hq, toks), hid_ref[...], NN)
    part = hq // n_dp
    for j in range(n_dp):
        w_own[j] = w[j * part:(j + 1) * part]
        w_send[j] = w[j * part:(j + 1) * part].astype(BF16)
    for off in range(1, n_dp):
        j = lax.rem(d + off, n_dp)
        slot_copy(w_send.at[j], w_recv, w_ss, w_rs, "dp", d, j).start()

    remote(0)

    total = w_own[d]
    for off in range(1, n_dp):
        j = lax.rem(d + off, n_dp)
        slot_copy(w_send.at[d], w_recv, w_ss, w_rs, "dp", j, d).wait_recv()
        total = total + w_recv[j].astype(F32)
    x_all[s] = total.astype(BF16)
    for off in range(1, n_seq):
        slot_copy(x_all.at[s], x_all, x_ss, x_rs, "seq", s, lax.rem(s + off, n_seq)).start()

    for k in range(1, kvh):
        remote(k)

    for off in range(1, n_seq):
        j = lax.rem(s + off, n_seq)
        slot_copy(x_all.at[j], x_all, x_ss, x_rs, "seq", j, s).wait_recv()
    total = x_all[0].astype(F32)
    for j in range(1, n_seq):
        total = total + x_all[j].astype(F32)
    o_all[d] = (total * (1.0 / math.sqrt(n_dp * n_seq * toks))).astype(BF16)
    for off in range(1, n_dp):
        slot_copy(o_all.at[d], o_all, o_ss, o_rs, "dp", d, lax.rem(d + off, n_dp)).start()

    for k in range(1, kvh):
        local(k)
    for t in range(tiles):
        qg_ref[t * blk:(t + 1) * blk] = jnp.concatenate(
            [dq_acc[t, k].reshape(blk, group, dh) for k in range(kvh)], axis=1
        ).__mul__(1.0 / root).astype(BF16)

    for k in range(kvh):
        kv_acc[k, 0] = (kv_acc[k, 0] * (1.0 / root)).astype(BF16).astype(F32)
        kv_acc[k, 1] = kv_acc[k, 1].astype(BF16).astype(F32)

        def add(j, k=k):
            g_copy(k, j, s).wait_recv()
            kv_acc[k] += g_recv[j, k].astype(F32)
        loop(s + 1, n_seq, add)
        dk_ref[k] = kv_acc[k, 0].astype(BF16)
        dv_ref[k] = kv_acc[k, 1].astype(BF16)

    for off in range(1, n_dp):
        j = lax.rem(d + off, n_dp)
        slot_copy(o_all.at[j], o_all, o_ss, o_rs, "dp", j, d).wait_recv()
    for j in range(n_dp):
        wg_ref[j] = o_all[j]

    for k in range(kvh):
        for c in range(2):
            loop(s + 1, n_seq, lambda j: kv_copy(k, c, s, j).wait_send())
        loop(0, s, lambda j: g_copy(k, s, j).wait_send())
    for off in range(1, n_head):
        slot_copy(lg_all.at[h], lg_all, lg_ss, lg_rs, "head", h, lax.rem(h + off, n_head)).wait_send()
    for off in range(1, n_dp):
        j = lax.rem(d + off, n_dp)
        slot_copy(w_send.at[j], w_recv, w_ss, w_rs, "dp", d, j).wait_send()
        slot_copy(o_all.at[d], o_all, o_ss, o_rs, "dp", d, j).wait_send()
    for off in range(1, n_seq):
        slot_copy(x_all.at[s], x_all, x_ss, x_rs, "seq", s, lax.rem(s + off, n_seq)).wait_send()


def finish(qg_ref, dk_ref, dv_ref, wg_ref, qo, ko, vo, wo, kbuf, vbuf, wbuf, sems):
    copies = [pltpu.make_async_copy(a, b, sems.at[i]) for i, (a, b) in enumerate(
        ((qg_ref, qo), (kbuf, ko), (vbuf, vo), (wbuf, wo)))]
    copies[0].start()
    part = wg_ref.shape[1]
    for j in range(wg_ref.shape[0]):
        wbuf[j * part:(j + 1) * part] = wg_ref[j].astype(F32)
    copies[3].start()
    for i, src, dst in ((1, dk_ref, kbuf), (2, dv_ref, vbuf)):
        dst[...] = jnp.concatenate(
            [src[k].astype(F32)[:, None, :] for k in range(src.shape[0])], axis=1).astype(BF16)
        copies[i].start()
    for c in copies:
        c.wait()


def on_device(
    queries, keys, values, attn_out, out_grad, gate_values, log_totals, hidden,
    block_ids, block_valid,
):
    toks, heads, dh = queries.shape[1:]
    kvh = keys.shape[2]
    tiles, nsel = block_ids.shape[1], block_ids.shape[3]
    group = heads // kvh
    blk = toks // tiles
    rows = blk * group
    n_seq, n_head, n_dp = (lax.axis_size(a) for a in ("seq", "head", "dp"))
    hq = n_head * heads
    width = hidden.shape[2]
    part = hq // n_dp
    dims = (n_seq, n_head, n_dp, tiles, blk, kvh, group, dh, nsel)
    any_ = pl.BlockSpec(memory_space=pl.ANY)
    vm = pl.BlockSpec(memory_space=pltpu.VMEM)
    sm = pl.BlockSpec(memory_space=pltpu.SMEM)
    dma = pltpu.SemaphoreType.DMA
    qg, dk, dv, wg = pl.pallas_call(
        functools.partial(kernel, dims),
        out_shape=(
            pltpu.VMEM((toks, heads, dh), BF16),
            pltpu.VMEM((kvh, toks, dh), BF16),
            pltpu.VMEM((kvh, toks, dh), BF16),
            pltpu.VMEM((n_dp, part, width), BF16),
        ),
        in_specs=[sm, sm] + [any_] * 4 + [vm] * 4,
        out_specs=(vm, vm, vm, vm),
        scratch_shapes=[
            pltpu.VMEM((toks, heads, dh), BF16),
            pltpu.VMEM((toks, heads, dh), BF16),
            pltpu.VMEM((toks, heads, dh), BF16),
            pltpu.VMEM((toks, width), BF16),
            pltpu.VMEM((kvh, toks, dh), BF16),
            pltpu.VMEM((kvh, toks, dh), BF16),
            dma((3, tiles)), dma,
            pltpu.VMEM((toks, 128), F32),
            pltpu.VMEM((toks, 128), F32),
            pltpu.VMEM((tiles, kvh, rows, 2 * dh), BF16),
            pltpu.VMEM((tiles, kvh, rows, 2 * dh), BF16),
            pltpu.VMEM((tiles, kvh, rows, dh), F32),
            pltpu.VMEM((n_seq, kvh, 2, toks, dh), BF16),
            pltpu.VMEM((kvh, 2, toks, dh), F32),
            pltpu.VMEM((n_seq, kvh, 2, toks, dh), BF16),
            pltpu.VMEM((n_seq, kvh, 2, toks, dh), BF16),
            pltpu.VMEM((n_head, heads, toks), BF16),
            pltpu.VMEM((n_dp, part, width), F32),
            pltpu.VMEM((n_dp, part, width), BF16),
            pltpu.VMEM((n_dp, part, width), BF16),
            pltpu.VMEM((n_seq, part, width), BF16),
            pltpu.VMEM((n_dp, part, width), BF16),
            dma((n_seq, kvh, 2)), dma((n_seq, kvh, 2)), dma((n_seq, kvh)), dma((n_seq, kvh)),
            dma((n_head,)), dma((n_head,)), dma((n_dp,)), dma((n_dp,)),
            dma((n_seq,)), dma((n_seq,)), dma((n_dp,)), dma((n_dp,)),
        ],
        compiler_params=pltpu.CompilerParams(
            collective_id=0, has_side_effects=True, vmem_limit_bytes=62 * 1024 * 1024),
        name="attention_backward",
    )(block_ids[0], block_valid[0], queries[0], attn_out[0], out_grad[0], hidden[0],
      gate_values[0], log_totals[0],
      keys[0], values[0])
    query_grad, key_grad, value_grad, weight_grad = pl.pallas_call(
        finish,
        out_shape=(
            jax.ShapeDtypeStruct((toks, heads, dh), BF16),
            jax.ShapeDtypeStruct((toks, kvh, dh), BF16),
            jax.ShapeDtypeStruct((toks, kvh, dh), BF16),
            jax.ShapeDtypeStruct((hq, width), F32),
        ),
        in_specs=[vm] * 4,
        out_specs=(any_,) * 4,
        scratch_shapes=[
            pltpu.VMEM((toks, kvh, dh), BF16),
            pltpu.VMEM((toks, kvh, dh), BF16),
            pltpu.VMEM((hq, width), F32),
            dma((4,)),
        ],
        compiler_params=pltpu.CompilerParams(vmem_limit_bytes=16 * 1024 * 1024),
        name="write_outputs",
    )(*(pltpu.with_memory_space_constraint(a, pltpu.VMEM) for a in (qg, dk, dv, wg)))
    return query_grad[None], key_grad[None], value_grad[None], weight_grad


def solution(mesh):
    return jax.shard_map(
        on_device,
        mesh=mesh,
        in_specs=(
            P("dp", "seq", "head", None),
            P("dp", "seq", "head", None),
            P("dp", "seq", "head", None),
            P("dp", "seq", "head", None),
            P("dp", "seq", "head", None),
            P("dp", "head", "seq"),
            P("dp", "head", "seq"),
            P("dp", "seq", "head"),
            P("dp", "seq", "head", None),
            P("dp", "seq", "head", None),
        ),
        out_specs=(
            P("dp", "seq", "head", None),
            P("dp", "seq", "head", None),
            P("dp", "seq", "head", None),
            P(None, "head"),
        ),
        check_vma=False,
    )
```
